16 devices in a mesh: lat: 2 (over z), dom: 2 (over y), ens: 4 (over x, core).
Axes of the slice: x: 2, y: 2, z: 2, core: 2. Of those that a mesh axis runs over, the one named last changes fastest.
Arguments:
- ens_state: bfloat16 [128, 16, 4096, 32], P('ens', 'lat', 'dom')
- w_in: bfloat16 [64, 128], replicated
- w_out: bfloat16 [128, 32], replicated
- obs_op: bfloat16 [32, 8], replicated
- obs_val: float32 [16, 16, 256, 8], P('lat', 'dom')
- obs_wt: float32 [16, 16, 256, 8], P('lat', 'dom')
Outputs:
- output: bfloat16 [128, 16, 4096, 32], P('ens', 'lat', 'dom')
All inputs are finite; a program needn't handle non-finite values.
Results may differ from the reference program's by a relative error of at most 0.001.
Values are sent between devices in bfloat16 or wider.
A program may use at most 1 GiB of HBM per device.

```python
import jax
import jax.numpy as jnp
from jax import lax

MEMBERS = 128
CHANNELS = 32
HIDDEN = 128
OBS_CHAN = 8
PATCH_LEN = 256
GRID_ROWS = 16
GRID_COLS = 4096
NS_STEPS = 12
TOP_PRECISION = lax.Precision.HIGHEST


def setup_inputs(seed: int = 0) -> dict:
    key_list = jax.random.split(jax.random.key(seed), 7)
    patch_count = GRID_COLS // PATCH_LEN
    mean_field = jax.random.normal(key_list[0], (GRID_ROWS, GRID_COLS, CHANNELS), jnp.float32)
    member_dev = 0.3 * jax.random.normal(key_list[1], (MEMBERS, GRID_ROWS, GRID_COLS, CHANNELS), jnp.float32)
    ens_state = (mean_field[None] + member_dev).astype(jnp.bfloat16)
    w_in = (jax.random.normal(key_list[2], (2 * CHANNELS, HIDDEN), jnp.float32) * (2 * CHANNELS) ** -0.5).astype(jnp.bfloat16)
    w_out = (jax.random.normal(key_list[3], (HIDDEN, CHANNELS), jnp.float32) * (0.5 * HIDDEN ** -0.5)).astype(jnp.bfloat16)
    obs_op = (jax.random.normal(key_list[4], (CHANNELS, OBS_CHAN), jnp.float32) * CHANNELS ** -0.5).astype(jnp.bfloat16)
    obs_shape = (GRID_ROWS, patch_count, PATCH_LEN, OBS_CHAN)
    obs_val = 1.5 * jax.random.normal(key_list[5], obs_shape, jnp.float32)
    obs_wt = jax.random.uniform(key_list[6], obs_shape, jnp.float32, 0.25, 1.75) * (MEMBERS / (PATCH_LEN * OBS_CHAN))
    return {'ens_state': ens_state, 'w_in': w_in, 'w_out': w_out, 'obs_op': obs_op, 'obs_val': obs_val, 'obs_wt': obs_wt}


def forecast_member(member, w_in, w_out):
    x_f32 = member.astype(jnp.float32)
    row_above = jnp.concatenate([x_f32[:1], x_f32[:-1]], axis=0)
    row_below = jnp.concatenate([x_f32[1:], x_f32[-1:]], axis=0)
    col_west = jnp.roll(x_f32, 1, axis=1)
    col_east = jnp.roll(x_f32, -1, axis=1)
    laplace = (row_above + row_below + col_west + col_east - 4.0 * x_f32).astype(jnp.bfloat16)
    features = jnp.concatenate([member, laplace], axis=-1).reshape(GRID_ROWS * GRID_COLS, 2 * CHANNELS)
    pre_act = jnp.dot(features, w_in, preferred_element_type=jnp.float32)
    hidden = jax.nn.gelu(pre_act, approximate=False).astype(jnp.bfloat16)
    update = jnp.dot(hidden, w_out, preferred_element_type=jnp.float32)
    return (x_f32 + update.reshape(GRID_ROWS, GRID_COLS, CHANNELS)).astype(jnp.bfloat16)


def inverse_root(a_mat):
    eye_mat = jnp.eye(MEMBERS, dtype=jnp.float32)
    scale_f = jnp.sqrt(jnp.sum(a_mat * a_mat, axis=(-2, -1), keepdims=True))

    def step_fn(carry, step_in):
        y_mat, z_mat = carry
        t_mat = 1.5 * eye_mat - 0.5 * jnp.einsum('nij,njk->nik', z_mat, y_mat, precision=TOP_PRECISION)
        y_next = jnp.einsum('nij,njk->nik', y_mat, t_mat, precision=TOP_PRECISION)
        z_next = jnp.einsum('nij,njk->nik', t_mat, z_mat, precision=TOP_PRECISION)
        return (y_next, z_next), None

    z_init = jnp.broadcast_to(eye_mat, a_mat.shape)
    final_pair, step_out = lax.scan(step_fn, (a_mat / scale_f, z_init), None, length=NS_STEPS)
    return final_pair[1] / jnp.sqrt(scale_f)


def analyse_row(xf_row, obs_row, wt_row, obs_op):
    n_patch = GRID_COLS // PATCH_LEN
    obs_width = PATCH_LEN * OBS_CHAN
    xf_pts = xf_row.astype(jnp.float32).reshape(MEMBERS, n_patch, PATCH_LEN, CHANNELS)
    x_mean = jnp.mean(xf_pts, axis=0)
    x_anom = xf_pts - x_mean
    y_back = jnp.einsum('enbc,co->enbo', xf_pts, obs_op.astype(jnp.float32), precision=TOP_PRECISION)
    y_mean = jnp.mean(y_back, axis=0)
    y_anom = (y_back - y_mean).reshape(MEMBERS, n_patch, obs_width)
    c_mat = y_anom * wt_row.reshape(n_patch, obs_width)
    a_mat = jnp.einsum('enq,fnq->nef', c_mat, y_anom, precision=TOP_PRECISION) + (MEMBERS - 1) * jnp.eye(MEMBERS, dtype=jnp.float32)
    s_mat = inverse_root(a_mat)
    pa_mat = jnp.einsum('nij,njk->nik', s_mat, s_mat, precision=TOP_PRECISION)
    innovation = obs_row.reshape(n_patch, obs_width) - y_mean.reshape(n_patch, obs_width)
    c_innov = jnp.einsum('enq,nq->ne', c_mat, innovation, precision=TOP_PRECISION)
    w_mean = jnp.einsum('nef,nf->ne', pa_mat, c_innov, precision=TOP_PRECISION)
    t_mat = (MEMBERS - 1) ** 0.5 * s_mat + w_mean[:, :, None]
    x_anal = x_mean + jnp.einsum('knbc,nke->enbc', x_anom, t_mat, precision=TOP_PRECISION)
    return x_anal.reshape(MEMBERS, GRID_COLS, CHANNELS).astype(jnp.bfloat16)


def reference(ens_state, w_in, w_out, obs_op, obs_val, obs_wt):
    forecast = lax.map(lambda member: forecast_member(member, w_in, w_out), ens_state)
    by_row = jnp.swapaxes(forecast, 0, 1)
    analysed = lax.map(lambda row_args: analyse_row(row_args[0], row_args[1], row_args[2], obs_op), (by_row, obs_val, obs_wt))
    return jnp.swapaxes(analysed, 0, 1)
```

```python
import functools
import math

import jax
import jax.numpy as jnp
from jax import lax
from jax.experimental import pallas as pl
from jax.experimental.pallas import tpu as pltpu
from jax.sharding import PartitionSpec as P

NS_STEPS = 12
HIGHEST = lax.Precision.HIGHEST
F32 = jnp.float32
BF16 = jnp.bfloat16
SQRT_HALF = math.sqrt(0.5)
MB = 16
BLOCK = 512
PATCH = 256
EDGE = 128


def dot(a, b, **kw):
    return jnp.dot(a, b, preferred_element_type=F32, **kw)


def halo_kernel(first_ref, last_ref, out_ref):
    members, rows, chans, lanes = first_ref.shape
    lane = lax.broadcasted_iota(jnp.int32, (chans, lanes), 1)

    def body(m, carry):
        acc = jnp.zeros((chans, lanes), F32)
        for r in range(rows):
            a = first_ref[m, r].astype(F32)
            b = last_ref[m, r].astype(F32)
            acc = jnp.where(lane == r, pltpu.roll(a, r, 1) if r else a, acc)
            acc = jnp.where(lane == rows + r, pltpu.roll(b, rows + r + 1, 1), acc)
        out_ref[m] = acc.astype(BF16)
        return carry

    lax.fori_loop(0, members, body, 0)


def make_halo(xt):
    members, rows, chans, cols = xt.shape
    step = 8
    spec = lambda j: pl.BlockSpec((step, rows, chans, EDGE), lambda i: (i, 0, 0, j))
    return pl.pallas_call(
        halo_kernel,
        grid=(members // step,),
        in_specs=[spec(0), spec(cols // EDGE - 1)],
        out_specs=pl.BlockSpec((step, chans, EDGE), lambda i: (i, 0, 0)),
        out_shape=jax.ShapeDtypeStruct((members, chans, EDGE), BF16),
        name="halo_pack",
    )(xt, xt)


def forecast_kernel(cfg, pos_ref, *refs):
    row, rows, wrap, west_lane, east_lane = cfg
    (x0, x1, u0, u1, d0, d1, nb_left, nb_right, col_ref, w1_ref, w2_ref, pm_ref, *outs, xl, xf) = refs
    chans = x0.shape[2]
    ens_i, lat_i = pos_ref[0], pos_ref[1]
    lane = lax.broadcasted_iota(jnp.int32, (MB, BLOCK), 1)

    def lap_body(m, carry):
        for h in range(chans // MB):
            s = slice(h * MB, (h + 1) * MB)
            halves = [x0[m, 0, s, :].astype(F32), x1[m, 0, s, :].astype(F32)]
            left_in = nb_left[m, 0, s, :].astype(F32)[:, EDGE - 1:]
            right_in = nb_right[m, 0, s, :].astype(F32)[:, :1]
            if wrap:
                col = col_ref[m, s, :].astype(F32)
                edges = [(left_in, col[:, east_lane:east_lane + 1]), (col[:, west_lane:west_lane + 1], right_in)]
            else:
                edges = [(left_in, halves[1][:, :1]), (halves[0][:, BLOCK - 1:], right_in)]
            for i in range(2):
                x = halves[i]
                u_ref, d_ref = (u0, d0) if i == 0 else (u1, d1)
                up, down = u_ref[m, 0, s, :].astype(F32), d_ref[m, 0, s, :].astype(F32)
                if row == 0:
                    up = jnp.where(lat_i == 0, x, up)
                if row == rows - 1:
                    down = jnp.where(lat_i == 0, down, x)
                west = jnp.where(lane == 0, edges[i][0], pltpu.roll(x, 1, 1))
                east = jnp.where(lane == BLOCK - 1, edges[i][1], pltpu.roll(x, BLOCK - 1, 1))
                lap = up + down + west + east - 4.0 * x
                c = slice(i * BLOCK, (i + 1) * BLOCK)
                xl[m, s, c] = x.astype(BF16)
                xl[m, chans + h * MB:chans + (h + 1) * MB, c] = lap.astype(BF16)
        return carry

    lax.fori_loop(0, MB, lap_body, 0)

    for k in range(4):
        off = pl.multiple_of((ens_i ^ k) * PATCH, PATCH)

        def mem_body(m, carry):
            feats = xl[m, :, pl.ds(off, PATCH)]
            pre = dot(w1_ref[...], feats)
            hid = ((0.5 * pre) * (1.0 + lax.erf(pre * SQRT_HALF))).astype(BF16)
            upd = dot(w2_ref[...], hid)
            xf[m] = (feats[:chans].astype(F32) + upd).astype(BF16)
            return carry

        lax.fori_loop(0, MB, mem_body, 0, unroll=4)
        for h in range(chans // MB):
            t = xf[:, h * MB:(h + 1) * MB, :].reshape(MB * MB, PATCH)
            outs[k][h * MB:(h + 1) * MB] = dot(pm_ref[...], t).astype(BF16).reshape(MB, MB, PATCH)


def forecast(xt, lat_halo, col_halo, w1t, w2t, perm, pos, row, kind):
    members, rows, chans, cols = xt.shape
    last = cols // BLOCK - 1
    wrap = kind == 1
    g0, g1 = (last, 0) if wrap else (1, 2)
    per = BLOCK // EDGE

    def xspec(r, g, width=BLOCK):
        return pl.BlockSpec((MB, 1, chans, width), lambda i, p: (i, r, 0, g))

    halo_spec = lambda g: pl.BlockSpec((MB, 1, chans, BLOCK), lambda i, p: (i, 0, 0, g))
    up_spec = (lambda g: halo_spec(g)) if row == 0 else (lambda g: xspec(row - 1, g))
    down_spec = (lambda g: halo_spec(g)) if row == rows - 1 else (lambda g: xspec(row + 1, g))
    up = lat_halo if row == 0 else xt
    down = lat_halo if row == rows - 1 else xt
    whole = lambda a: pl.BlockSpec(a.shape, lambda i, p: (0,) * a.ndim)
    piece = jax.ShapeDtypeStruct((chans, members, PATCH), BF16)
    return pl.pallas_call(
        functools.partial(forecast_kernel, (row, rows, wrap, rows + row, row)),
        grid_spec=pltpu.PrefetchScalarGridSpec(
            num_scalar_prefetch=1,
            grid=(members // MB,),
            in_specs=[
                xspec(row, g0), xspec(row, g1), up_spec(g0), up_spec(g1), down_spec(g0), down_spec(g1),
                xspec(row, g0 * per - 1, EDGE), xspec(row, (g1 + 1) * per, EDGE),
                pl.BlockSpec((MB, chans, EDGE), lambda i, p: (i, 0, 0)),
                whole(w1t), whole(w2t), whole(perm),
            ],
            out_specs=[pl.BlockSpec((chans, MB, PATCH), lambda i, p: (0, i, 0))] * 4,
            scratch_shapes=[pltpu.VMEM((MB, 2 * chans, 2 * BLOCK), BF16), pltpu.VMEM((MB, chans, PATCH), BF16)],
        ),
        out_shape=[piece] * 4,
        name=f"forecast_{row}_{kind}",
    )(pos, xt, xt, up, up, down, down, xt, xt, col_halo, w1t, w2t, perm)


def analysis_kernel(pos_ref, r0, r1, r2, r3, yo_ref, wt_ref, kh_ref, pm_ref, o0, o1, o2, o3, yb, xa, ys, zs):
    ins, outs = (r0, r1, r2, r3), (o0, o1, o2, o3)
    chans, group = r0.shape[0], r0.shape[1]
    obs = yo_ref.shape[2]
    count = 4 * group
    for k in range(4):
        for j in range(group // MB):
            y = jnp.zeros((obs * MB, PATCH), F32)
            for h in range(chans // MB):
                t = ins[k][h * MB:(h + 1) * MB, j * MB:(j + 1) * MB, :].reshape(MB * MB, PATCH)
                y = y + dot(kh_ref[h], t)
            e0 = k * group + j * MB
            yb[:, e0:e0 + MB, :] = y.reshape(obs, MB, PATCH)
    a = jnp.zeros((count, count), F32)
    ci = jnp.zeros((count, PATCH), F32)
    for o in range(obs):
        y = yb[o]
        mean = jnp.sum(y, axis=0, keepdims=True) * (1.0 / count)
        yp = y - mean
        cm = yp * wt_ref[0, 0, o:o + 1, :]
        a = a + lax.dot_general(cm, yp, (((1,), (1,)), ((), ())), precision=HIGHEST, preferred_element_type=F32)
        ci = ci + cm * (yo_ref[0, 0, o:o + 1, :] - mean)
    rid = lax.broadcasted_iota(jnp.int32, (count, count), 0)
    cid = lax.broadcasted_iota(jnp.int32, (count, count), 1)
    eye = jnp.where(rid == cid, 1.0, 0.0).astype(F32)
    a = a + (count - 1.0) * eye
    scale = jnp.sqrt(jnp.sum(jnp.sum(a * a, axis=1, keepdims=True), axis=0, keepdims=True))
    y = a / scale
    t = 1.5 * eye - 0.5 * y
    ys[...], zs[...] = dot(y, t, precision=HIGHEST), t

    def step(i, carry):
        t = 1.5 * eye - 0.5 * dot(zs[...], ys[...], precision=HIGHEST)
        ys[...], zs[...] = dot(ys[...], t, precision=HIGHEST), dot(t, zs[...], precision=HIGHEST)
        return carry

    lax.fori_loop(0, NS_STEPS - 2, step, 0)
    t = 1.5 * eye - 0.5 * dot(zs[...], ys[...], precision=HIGHEST)
    z = dot(t, zs[...], precision=HIGHEST)
    s = z / jnp.sqrt(scale)
    cb = jnp.broadcast_to(jnp.sum(ci, axis=1, keepdims=True), (count, count))
    wbar = dot(s, dot(s, cb, precision=HIGHEST), precision=HIGHEST)
    t = math.sqrt(count - 1) * s + wbar
    m = t + (1.0 - jnp.sum(t, axis=0, keepdims=True)) * (1.0 / count)
    m = m.T
    m1 = m.astype(BF16)
    rest = m - m1.astype(F32)
    m2 = rest.astype(BF16)
    m3 = (rest - m2.astype(F32)).astype(BF16)

    def chan_body(c, carry):
        x = jnp.concatenate([ins[k][c] for k in range(4)], axis=0)
        xa[c] = (dot(m1, x) + (dot(m2, x) + dot(m3, x))).astype(BF16)
        return carry

    lax.fori_loop(0, chans, chan_body, 0, unroll=4)
    for k in range(4):
        for j in range(group // MB):
            e0 = k * group + j * MB
            for h in range(chans // MB):
                t = xa[h * MB:(h + 1) * MB, e0:e0 + MB, :].reshape(MB * MB, PATCH)
                outs[k][j * MB:(j + 1) * MB, h * MB:(h + 1) * MB, :] = dot(pm_ref[...], t).astype(BF16).reshape(MB, MB, PATCH)


def patch_of(kind, pos, patches):
    return pos + patches // 4 if kind == 0 else lax.rem(pos + 3 * (patches // 4), patches)


def analyse(pieces, obs_v, obs_w, kh, perm, pos, row, kind):
    chans, group, _ = pieces[0].shape
    patches, obs = obs_v.shape[1:3]
    whole = lambda a: pl.BlockSpec(a.shape, lambda i, p: (0,) * a.ndim)
    ospec = pl.BlockSpec((1, 1, obs, PATCH), lambda i, p: (row, patch_of(kind, p[0], patches), 0, 0))
    piece = jax.ShapeDtypeStruct((group, chans, PATCH), BF16)
    return pl.pallas_call(
        analysis_kernel,
        grid_spec=pltpu.PrefetchScalarGridSpec(
            num_scalar_prefetch=1,
            grid=(1,),
            in_specs=[whole(a) for a in pieces] + [ospec, ospec, whole(kh), whole(perm)],
            out_specs=[whole(piece)] * 4,
            scratch_shapes=[pltpu.VMEM((obs, 4 * group, PATCH), F32), pltpu.VMEM((chans, 4 * group, PATCH), BF16)] + [pltpu.VMEM((4 * group, 4 * group), F32)] * 2,
        ),
        out_shape=[piece] * 4,
        name=f"analysis_{row}_{kind}",
    )(pos, *pieces, obs_v, obs_w, kh, perm)


def write_kernel(pos_ref, p0, p1, p2, p3, *rest):
    out = rest[-1]
    for k, ref in enumerate((p0, p1, p2, p3)):
        @pl.when(pl.program_id(0) == k)
        def _():
            out[...] = ref[...].reshape(out.shape)


def write(out, pieces, shape, pos, row, kind):
    group, chans, _ = pieces[0].shape
    patches = shape[3] // PATCH
    whole = lambda a: pl.BlockSpec(a.shape, lambda i, p: (0,) * a.ndim)
    first = out is None
    return pl.pallas_call(
        write_kernel,
        grid_spec=pltpu.PrefetchScalarGridSpec(
            num_scalar_prefetch=1,
            grid=(4,),
            in_specs=[whole(a) for a in pieces] + ([] if first else [pl.BlockSpec(memory_space=pl.ANY)]),
            out_specs=pl.BlockSpec((group, 1, chans, PATCH), lambda i, p: (0, row, 0, patch_of(kind, p[0] ^ i, patches))),
        ),
        out_shape=jax.ShapeDtypeStruct(shape, BF16),
        input_output_aliases={} if first else {5: 0},
        name=f"write_{row}_{kind}",
    )(pos, *pieces, *([] if first else [out]))


def solution(mesh):
    ens = mesh.shape['ens']
    assert ens == 4 and mesh.shape['lat'] == 2 and mesh.shape['dom'] == 2
    swap = [(0, 1), (1, 0)]

    def exchange(pieces):
        return [pieces[0]] + [lax.ppermute(pieces[k], 'ens', [(s, s ^ k) for s in range(ens)]) for k in range(1, ens)]

    def local_cycle(ens_block, w_in, w_out, obs_op, obs_val, obs_wt):
        xt = ens_block.transpose(0, 1, 3, 2)
        members, rows, chans, cols = xt.shape
        obs_v, obs_w = obs_val.transpose(0, 1, 3, 2), obs_wt.transpose(0, 1, 3, 2)
        lat_i, ens_i = lax.axis_index('lat'), lax.axis_index('ens')
        pos = jnp.stack([ens_i, lat_i]).astype(jnp.int32)
        w1t, w2t = w_in.T, w_out.T
        i0 = lax.broadcasted_iota(jnp.int32, (MB * MB, MB * MB), 0)
        i1 = lax.broadcasted_iota(jnp.int32, (MB * MB, MB * MB), 1)
        perm = (i1 == (i0 % MB) * MB + i0 // MB).astype(BF16)
        obs = obs_op.shape[1]
        eye = jnp.eye(MB, dtype=BF16)
        kh = jnp.einsum('hco,ed->hoecd', obs_op.reshape(chans // MB, MB, obs), eye).reshape(chans // MB, obs * MB, MB * MB)
        col_halo = lax.ppermute(make_halo(xt), 'dom', swap)
        edge_row = lax.dynamic_slice_in_dim(xt, (1 - lat_i) * (rows - 1), 1, axis=1)
        lat_halo = lax.ppermute(edge_row, 'lat', swap)

        chunks = [(r, kind) for r in list(range(1, rows - 1)) + [0, rows - 1] for kind in (0, 1)]
        fields = [forecast(xt, lat_halo, col_halo, w1t, w2t, perm, pos, r, kind) for r, kind in chunks]
        fields = [exchange(f) for f in fields]
        analysed = [analyse(f, obs_v, obs_w, kh, perm, pos, r, kind) for f, (r, kind) in zip(fields, chunks)]
        analysed = [exchange(f) for f in analysed]
        out = None
        for f, (r, kind) in zip(analysed, chunks):
            out = write(out, f, xt.shape, pos, r, kind)
        return out.transpose(0, 1, 3, 2)

    state_spec = P('ens', 'lat', 'dom', None)
    obs_spec = P('lat', 'dom', None, None)
    return jax.shard_map(local_cycle, mesh=mesh, in_specs=(state_spec, P(), P(), P(), obs_spec, obs_spec), out_specs=state_spec, check_vma=False)
```

```python
import functools
import math

import jax
import jax.numpy as jnp
from jax import lax
from jax.experimental import pallas as pl
from jax.experimental.pallas import tpu as pltpu
from jax.sharding import PartitionSpec as P

NS_STEPS = 12
HIGHEST = lax.Precision.HIGHEST
F32 = jnp.float32
BF16 = jnp.bfloat16
SQRT_HALF = math.sqrt(0.5)
MB = 16
BLOCK = 512
PATCH = 256
EDGE = 128


def dot(a, b, **kw):
    return jnp.dot(a, b, preferred_element_type=F32, **kw)


def halo_kernel(first_ref, last_ref, after_ref, out_ref):
    members, rows, chans, lanes = first_ref.shape
    lane = lax.broadcasted_iota(jnp.int32, (chans, lanes), 1)

    def body(m, carry):
        acc = jnp.zeros((chans, lanes), F32)
        for r in range(rows):
            a = first_ref[m, r].astype(F32)
            b = last_ref[m, r].astype(F32)
            acc = jnp.where(lane == r, pltpu.roll(a, r, 1) if r else a, acc)
            acc = jnp.where(lane == rows + r, pltpu.roll(b, rows + r + 1, 1), acc)
        out_ref[m] = acc.astype(BF16)
        return carry

    lax.fori_loop(0, members, body, 0)


def make_halo(xt, after):
    members, rows, chans, cols = xt.shape
    step = 8
    spec = lambda j: pl.BlockSpec((step, rows, chans, EDGE), lambda i: (i, 0, 0, j))
    return pl.pallas_call(
        halo_kernel,
        grid=(members // step,),
        in_specs=[spec(0), spec(cols // EDGE - 1), pl.BlockSpec(memory_space=pl.ANY)],
        out_specs=pl.BlockSpec((step, chans, EDGE), lambda i: (i, 0, 0)),
        out_shape=jax.ShapeDtypeStruct((members, chans, EDGE), BF16),
        name="halo_pack",
    )(xt, xt, after)


def forecast_kernel(cfg, pos_ref, *refs):
    row, rows, wrap, west_lane, east_lane, chained = cfg
    (x0, x1, u0, u1, d0, d1, nb_left, nb_right, w1_ref, w2_ref, pm_ref), refs = refs[:11], refs[11 + chained:]
    col_ref, refs = (refs[0], refs[1:]) if wrap else (None, refs)
    *outs, xl, xf, hid = refs
    chans = x0.shape[2]
    ens_i, lat_i = pos_ref[0], pos_ref[1]
    lane = lax.broadcasted_iota(jnp.int32, (MB, BLOCK), 1)

    def lap_body(m, carry):
        for h in range(chans // MB):
            s = slice(h * MB, (h + 1) * MB)
            halves = [x0[m, 0, s, :].astype(F32), x1[m, 0, s, :].astype(F32)]
            left_in = nb_left[m, 0, s, :].astype(F32)[:, EDGE - 1:]
            right_in = nb_right[m, 0, s, :].astype(F32)[:, :1]
            if wrap:
                col = col_ref[m, s, :].astype(F32)
                edges = [(left_in, col[:, east_lane:east_lane + 1]), (col[:, west_lane:west_lane + 1], right_in)]
            else:
                edges = [(left_in, halves[1][:, :1]), (halves[0][:, BLOCK - 1:], right_in)]
            for i in range(2):
                x = halves[i]
                u_ref, d_ref = (u0, d0) if i == 0 else (u1, d1)
                up, down = u_ref[m, 0, s, :].astype(F32), d_ref[m, 0, s, :].astype(F32)
                if row == 0:
                    up = jnp.where(lat_i == 0, x, up)
                if row == rows - 1:
                    down = jnp.where(lat_i == 0, down, x)
                west = jnp.where(lane == 0, edges[i][0], pltpu.roll(x, 1, 1))
                east = jnp.where(lane == BLOCK - 1, edges[i][1], pltpu.roll(x, BLOCK - 1, 1))
                lap = up + down + west + east - 4.0 * x
                c = slice(i * BLOCK, (i + 1) * BLOCK)
                xl[m, s, c] = x.astype(BF16)
                xl[m, chans + h * MB:chans + (h + 1) * MB, c] = lap.astype(BF16)
        return carry

    lax.fori_loop(0, MB, lap_body, 0)

    tiles = [slice(t * PATCH, (t + 1) * PATCH) for t in range(4)]

    def first_dots(m):
        return [dot(w1_ref[...], xl[m, :, t]) for t in tiles]

    def second_dots(b):
        return [dot(w2_ref[...], hid[b, :, t]) for t in tiles]

    def store_hidden(b, pres):
        for t, pre in zip(tiles, pres):
            hid[b, :, t] = ((0.5 * pre) * (1.0 + lax.erf(pre * SQRT_HALF))).astype(BF16)

    def store_field(m, upds):
        for t, upd in zip(tiles, upds):
            xf[m, :, t] = (xl[m, :chans, t].astype(F32) + upd).astype(BF16)

    def both(m, b):
        pres = first_dots(m)
        upds = second_dots(1 - b)
        store_hidden(b, pres)
        store_field(m - 1, upds)

    store_hidden(0, first_dots(0))

    def pair_body(i, carry):
        both(2 * i + 1, 1)
        both(2 * i + 2, 0)
        return carry

    lax.fori_loop(0, MB // 2 - 1, pair_body, 0)
    both(MB - 1, 1)
    store_field(MB - 1, second_dots(1))

    for k in range(4):
        off = pl.multiple_of((ens_i ^ k) * PATCH, PATCH)
        for h in range(chans // MB):
            t = xf[:, h * MB:(h + 1) * MB, pl.ds(off, PATCH)].reshape(MB * MB, PATCH)
            outs[k][h * MB:(h + 1) * MB] = dot(pm_ref[...], t).astype(BF16).reshape(MB, MB, PATCH)


def forecast(xt, lat_halo, col_halo, w1t, w2t, perm, pos, row, kind, after=()):
    members, rows, chans, cols = xt.shape
    last = cols // BLOCK - 1
    wrap = kind == 1
    g0, g1 = (last, 0) if wrap else (1, 2)
    per = BLOCK // EDGE

    def xspec(r, g, width=BLOCK):
        return pl.BlockSpec((MB, 1, chans, width), lambda i, p: (i, r, 0, g))

    halo_spec = lambda g: pl.BlockSpec((MB, 1, chans, BLOCK), lambda i, p: (i, 0, 0, g))
    up_spec = (lambda g: halo_spec(g)) if row == 0 else (lambda g: xspec(row - 1, g))
    down_spec = (lambda g: halo_spec(g)) if row == rows - 1 else (lambda g: xspec(row + 1, g))
    up = lat_halo if row == 0 else xt
    down = lat_halo if row == rows - 1 else xt
    whole = lambda a: pl.BlockSpec(a.shape, lambda i, p: (0,) * a.ndim)
    piece = jax.ShapeDtypeStruct((chans, members, PATCH), BF16)
    return pl.pallas_call(
        functools.partial(forecast_kernel, (row, rows, wrap, rows + row, row, len(after))),
        grid_spec=pltpu.PrefetchScalarGridSpec(
            num_scalar_prefetch=1,
            grid=(members // MB,),
            in_specs=[
                xspec(row, g0), xspec(row, g1), up_spec(g0), up_spec(g1), down_spec(g0), down_spec(g1),
                xspec(row, g0 * per - 1, EDGE), xspec(row, (g1 + 1) * per, EDGE),
                whole(w1t), whole(w2t), whole(perm),
            ] + [pl.BlockSpec(memory_space=pl.ANY)] * len(after) + ([pl.BlockSpec((MB, chans, EDGE), lambda i, p: (i, 0, 0))] if wrap else []),
            out_specs=[pl.BlockSpec((chans, MB, PATCH), lambda i, p: (0, i, 0))] * 4,
            scratch_shapes=[pltpu.VMEM((MB, 2 * chans, 2 * BLOCK), BF16), pltpu.VMEM((MB, chans, 2 * BLOCK), BF16), pltpu.VMEM((2, w1t.shape[0], 2 * BLOCK), BF16)],
        ),
        out_shape=[piece] * 4,
        name=f"forecast_{row}_{kind}",
    )(pos, xt, xt, up, up, down, down, xt, xt, w1t, w2t, perm, *after, *([col_halo] if wrap else []))


def analysis_kernel(pos_ref, r0, r1, r2, r3, yo_ref, wt_ref, kh_ref, pm_ref, o0, o1, o2, o3, yb, xa, ys, zs):
    ins, outs = (r0, r1, r2, r3), (o0, o1, o2, o3)
    chans, group = r0.shape[0], r0.shape[1]
    obs = yo_ref.shape[2]
    count = 4 * group
    for k in range(4):
        for j in range(group // MB):
            y = jnp.zeros((obs * MB, PATCH), F32)
            for h in range(chans // MB):
                t = ins[k][h * MB:(h + 1) * MB, j * MB:(j + 1) * MB, :].reshape(MB * MB, PATCH)
                y = y + dot(kh_ref[h], t)
            e0 = k * group + j * MB
            yb[:, e0:e0 + MB, :] = y.reshape(obs, MB, PATCH)
    a = jnp.zeros((count, count), F32)
    ci = jnp.zeros((count, PATCH), F32)
    for o in range(obs):
        y = yb[o]
        mean = jnp.sum(y, axis=0, keepdims=True) * (1.0 / count)
        yp = y - mean
        cm = yp * wt_ref[0, 0, o:o + 1, :]
        a = a + lax.dot_general(cm, yp, (((1,), (1,)), ((), ())), precision=HIGHEST, preferred_element_type=F32)
        ci = ci + cm * (yo_ref[0, 0, o:o + 1, :] - mean)
    rid = lax.broadcasted_iota(jnp.int32, (count, count), 0)
    cid = lax.broadcasted_iota(jnp.int32, (count, count), 1)
    eye = jnp.where(rid == cid, 1.0, 0.0).astype(F32)
    a = a + (count - 1.0) * eye
    scale = jnp.sqrt(jnp.sum(jnp.sum(a * a, axis=1, keepdims=True), axis=0, keepdims=True))
    y = a / scale
    t = 1.5 * eye - 0.5 * y
    ys[...], zs[...] = dot(y, t, precision=HIGHEST), t

    def step(i, carry):
        t = 1.5 * eye - 0.5 * dot(zs[...], ys[...], precision=HIGHEST)
        ys[...], zs[...] = dot(ys[...], t, precision=HIGHEST), dot(t, zs[...], precision=HIGHEST)
        return carry

    lax.fori_loop(0, NS_STEPS - 2, step, 0)
    t = 1.5 * eye - 0.5 * dot(zs[...], ys[...], precision=HIGHEST)
    z = dot(t, zs[...], precision=HIGHEST)
    s = z / jnp.sqrt(scale)
    cb = jnp.broadcast_to(jnp.sum(ci, axis=1, keepdims=True), (count, count))
    wbar = dot(s, dot(s, cb, precision=HIGHEST), precision=HIGHEST)
    t = math.sqrt(count - 1) * s + wbar
    m = t + (1.0 - jnp.sum(t, axis=0, keepdims=True)) * (1.0 / count)
    m = m.T
    m1 = m.astype(BF16)
    rest = m - m1.astype(F32)
    m2 = rest.astype(BF16)
    m3 = (rest - m2.astype(F32)).astype(BF16)

    def chan_body(c, carry):
        x = jnp.concatenate([ins[k][c] for k in range(4)], axis=0)
        xa[c] = (dot(m1, x) + (dot(m2, x) + dot(m3, x))).astype(BF16)
        return carry

    lax.fori_loop(0, chans, chan_body, 0, unroll=4)
    for k in range(4):
        for j in range(group // MB):
            e0 = k * group + j * MB
            for h in range(chans // MB):
                t = xa[h * MB:(h + 1) * MB, e0:e0 + MB, :].reshape(MB * MB, PATCH)
                outs[k][j * MB:(j + 1) * MB, h * MB:(h + 1) * MB, :] = dot(pm_ref[...], t).astype(BF16).reshape(MB, MB, PATCH)


def patch_of(kind, pos, patches):
    return pos + patches // 4 if kind == 0 else lax.rem(pos + 3 * (patches // 4), patches)


def analyse(pieces, obs_v, obs_w, kh, perm, pos, row, kind):
    chans, group, _ = pieces[0].shape
    patches, obs = obs_v.shape[1:3]
    whole = lambda a: pl.BlockSpec(a.shape, lambda i, p: (0,) * a.ndim)
    ospec = pl.BlockSpec((1, 1, obs, PATCH), lambda i, p: (row, patch_of(kind, p[0], patches), 0, 0))
    piece = jax.ShapeDtypeStruct((group, chans, PATCH), BF16)
    return pl.pallas_call(
        analysis_kernel,
        grid_spec=pltpu.PrefetchScalarGridSpec(
            num_scalar_prefetch=1,
            grid=(1,),
            in_specs=[whole(a) for a in pieces] + [ospec, ospec, whole(kh), whole(perm)],
            out_specs=[whole(piece)] * 4,
            scratch_shapes=[pltpu.VMEM((obs, 4 * group, PATCH), F32), pltpu.VMEM((chans, 4 * group, PATCH), BF16)] + [pltpu.VMEM((4 * group, 4 * group), F32)] * 2,
        ),
        out_shape=[piece] * 4,
        name=f"analysis_{row}_{kind}",
    )(pos, *pieces, obs_v, obs_w, kh, perm)


def write_kernel(pos_ref, p0, p1, p2, p3, *rest):
    out = rest[-1]
    for k, ref in enumerate((p0, p1, p2, p3)):
        @pl.when(pl.program_id(0) == k)
        def _():
            out[...] = ref[...].reshape(out.shape)


def write(out, pieces, shape, pos, row, kind):
    group, chans, _ = pieces[0].shape
    patches = shape[3] // PATCH
    whole = lambda a: pl.BlockSpec(a.shape, lambda i, p: (0,) * a.ndim)
    first = out is None
    return pl.pallas_call(
        write_kernel,
        grid_spec=pltpu.PrefetchScalarGridSpec(
            num_scalar_prefetch=1,
            grid=(4,),
            in_specs=[whole(a) for a in pieces] + ([] if first else [pl.BlockSpec(memory_space=pl.ANY)]),
            out_specs=pl.BlockSpec((group, 1, chans, PATCH), lambda i, p: (0, row, 0, patch_of(kind, p[0] ^ i, patches))),
        ),
        out_shape=jax.ShapeDtypeStruct(shape, BF16),
        input_output_aliases={} if first else {5: 0},
        name=f"write_{row}_{kind}",
    )(pos, *pieces, *([] if first else [out]))


def solution(mesh):
    ens = mesh.shape['ens']
    assert ens == 4 and mesh.shape['lat'] == 2 and mesh.shape['dom'] == 2
    swap = [(0, 1), (1, 0)]

    def exchange(pieces):
        return [pieces[0]] + [lax.ppermute(pieces[k], 'ens', [(s, s ^ k) for s in range(ens)]) for k in range(1, ens)]

    def local_cycle(ens_block, w_in, w_out, obs_op, obs_val, obs_wt):
        xt = ens_block.transpose(0, 1, 3, 2)
        members, rows, chans, cols = xt.shape
        obs_v, obs_w = obs_val.transpose(0, 1, 3, 2), obs_wt.transpose(0, 1, 3, 2)
        lat_i, ens_i = lax.axis_index('lat'), lax.axis_index('ens')
        pos = jnp.stack([ens_i, lat_i]).astype(jnp.int32)
        w1t, w2t = w_in.T, w_out.T
        i0 = lax.broadcasted_iota(jnp.int32, (MB * MB, MB * MB), 0)
        i1 = lax.broadcasted_iota(jnp.int32, (MB * MB, MB * MB), 1)
        perm = (i1 == (i0 % MB) * MB + i0 // MB).astype(BF16)
        obs = obs_op.shape[1]
        eye = jnp.eye(MB, dtype=BF16)
        kh = jnp.einsum('hco,ed->hoecd', obs_op.reshape(chans // MB, MB, obs), eye).reshape(chans // MB, obs * MB, MB * MB)
        inner = list(range(1, rows - 1))
        chunks = [(r, 0) for r in inner] + [(r, 1) for r in inner] + [(r, kind) for r in (0, rows - 1) for kind in (0, 1)]
        fields, col_halo, lat_halo = [], None, None
        for r, kind in chunks:
            after = [fields[-1][0]] if fields else []
            fields.append(forecast(xt, lat_halo, col_halo, w1t, w2t, perm, pos, r, kind, after))
            if len(fields) == 2:
                col_halo = lax.ppermute(make_halo(xt, fields[1][0]), 'dom', swap)
                edge, _ = lax.optimization_barrier(((1 - lat_i) * (rows - 1), fields[1][1]))
                lat_halo = lax.ppermute(lax.dynamic_slice_in_dim(xt, edge, 1, axis=1), 'lat', swap)
        fields = [exchange(f) for f in fields]
        analysed = [analyse(f, obs_v, obs_w, kh, perm, pos, r, kind) for f, (r, kind) in zip(fields, chunks)]
        analysed = [exchange(f) for f in analysed]
        out = None
        for f, (r, kind) in zip(analysed, chunks):
            out = write(out, f, xt.shape, pos, r, kind)
        return out.transpose(0, 1, 3, 2)

    state_spec = P('ens', 'lat', 'dom', None)
    obs_spec = P('lat', 'dom', None, None)
    return jax.shard_map(local_cycle, mesh=mesh, in_specs=(state_spec, P(), P(), P(), obs_spec, obs_spec), out_specs=state_spec, check_vma=False)
```
